128 devices in a mesh: dp: 1, tp: 2 (over core), ep: 64 (over z, y, x).
Axes of the slice: x: 4, y: 4, z: 4, core: 2. Of those that a mesh axis runs over, the one named last changes fastest.
Arguments:
- act_in: bfloat16 [262144, 768], P(('dp', 'ep'))
- expert_idx: int32 [262144, 1], P(('dp', 'ep'))
- gate_vals: float32 [262144, 1], P(('dp', 'ep'))
- w_in: bfloat16 [64, 768, 3072], P('ep', None, 'tp')
- w_out: bfloat16 [64, 3072, 768], P('ep', 'tp')
Outputs:
- output: bfloat16 [262144, 768], P(('dp', 'ep'))
All inputs are finite; a program needn't handle non-finite values.
Results may differ from the reference program's by a relative error of at most 0.001.
Values are sent between devices in bfloat16 or wider.
A program may use at most 1 GiB of HBM per device.

```python
import jax
import jax.numpy as jnp
from jax import lax

SOURCES = 64
TOKENS_DEV = 4096
HIDDEN = 768
FF_DIM = 3072
EXPERTS = 64
TOP_K = 1
CAPACITY = 80
NUM_TOK = SOURCES * TOKENS_DEV
NUM_SLOTS = EXPERTS * SOURCES * CAPACITY


def draw_routing(rng_key):
    key_first, key_gap, key_hot = jax.random.split(rng_key, 3)
    first_ids = jax.random.randint(key_first, (SOURCES, TOKENS_DEV), 0, EXPERTS, jnp.int32)
    hot_ids = jax.random.randint(key_hot, (SOURCES, 1), 0, EXPERTS, jnp.int32)
    forced = jnp.arange(TOKENS_DEV)[None, :] < CAPACITY + 8
    first_ids = jnp.where(forced, hot_ids, first_ids)
    gap_sizes = jax.random.randint(key_gap, (SOURCES, TOKENS_DEV, TOP_K - 1), 1, EXPERTS // TOP_K + 1, jnp.int32)
    offsets = jnp.concatenate([jnp.zeros((SOURCES, TOKENS_DEV, 1), jnp.int32), jnp.cumsum(gap_sizes, axis=2)], axis=2)
    return ((first_ids[:, :, None] + offsets) % EXPERTS).reshape(NUM_TOK, TOP_K).astype(jnp.int32)


def setup_inputs(seed: int = 0, part: int = 0) -> dict:
    weight_keys = jax.random.split(jax.random.key(seed), 2)
    w_in = (jax.random.normal(weight_keys[0], (EXPERTS, HIDDEN, FF_DIM), jnp.float32) * HIDDEN ** -0.5).astype(jnp.bfloat16)
    w_out = (jax.random.normal(weight_keys[1], (EXPERTS, FF_DIM, HIDDEN), jnp.float32) * FF_DIM ** -0.5).astype(jnp.bfloat16)
    part_keys = jax.random.split(jax.random.fold_in(jax.random.key(seed + 1), part), 3)
    act_in = jax.random.normal(part_keys[0], (NUM_TOK, HIDDEN), jnp.float32).astype(jnp.bfloat16)
    expert_idx = draw_routing(part_keys[1])
    gate_vals = jax.random.uniform(part_keys[2], (NUM_TOK, TOP_K), jnp.float32, 0.5, 1.5) * TOP_K ** -0.5
    return {"act_in": act_in, "expert_idx": expert_idx, "gate_vals": gate_vals, "w_in": w_in, "w_out": w_out}


def slot_ids_of(src_idx):
    hit_mask = src_idx[:, :, :, None] == jnp.arange(EXPERTS)
    per_tok = jnp.sum(hit_mask, axis=2, dtype=jnp.int32)
    preceding = jnp.cumsum(per_tok, axis=1) - per_tok
    return jnp.sum(jnp.where(hit_mask, preceding[:, :, None, :], 0), axis=3)


def reference(act_in, expert_idx, gate_vals, w_in, w_out):
    src_idx = expert_idx.reshape(SOURCES, TOKENS_DEV, TOP_K)
    slot_ids = slot_ids_of(src_idx)
    src_ids = jnp.arange(SOURCES)[:, None, None]
    slot_pos = jnp.where(slot_ids < CAPACITY, (src_idx * SOURCES + src_ids) * CAPACITY + slot_ids, NUM_SLOTS).reshape(-1)
    tok_ids = jnp.broadcast_to(src_ids * TOKENS_DEV + jnp.arange(TOKENS_DEV)[None, :, None], src_idx.shape).reshape(-1)
    tok_table = jnp.full((NUM_SLOTS + 1,), NUM_TOK, jnp.int32).at[slot_pos].set(tok_ids)[:NUM_SLOTS]
    gate_table = jnp.zeros((NUM_SLOTS + 1,), jnp.float32).at[slot_pos].set(gate_vals.reshape(-1))[:NUM_SLOTS]
    padded = jnp.concatenate([act_in, jnp.zeros((1, HIDDEN), act_in.dtype)], axis=0)

    def one_expert(acc_rows, packed):
        w_first, w_second, tok_rows, gate_rows = packed
        expert_rows = padded[tok_rows]
        pre_act = jnp.dot(expert_rows, w_first, preferred_element_type=jnp.float32)
        hidden_act = jax.nn.gelu(pre_act, approximate=True).astype(jnp.bfloat16)
        expert_out = jnp.dot(hidden_act, w_second, preferred_element_type=jnp.float32).astype(jnp.bfloat16)
        acc_rows = acc_rows.at[tok_rows].add(gate_rows[:, None] * expert_out.astype(jnp.float32))
        return acc_rows, None

    packed_all = (w_in, w_out, tok_table.reshape(EXPERTS, SOURCES * CAPACITY), gate_table.reshape(EXPERTS, SOURCES * CAPACITY))
    summed_rows = lax.scan(one_expert, jnp.zeros((NUM_TOK + 1, HIDDEN), jnp.float32), packed_all)[0]
    return summed_rows[:NUM_TOK].astype(jnp.bfloat16)
```

```python
import functools

import jax
import jax.numpy as jnp
from jax import lax
from jax.experimental import pallas as pl
from jax.experimental.pallas import tpu as pltpu
from jax.sharding import PartitionSpec as P

MESH = pl.DeviceIdType.MESH
SIDE = 4
CHIPS = SIDE ** 3
SUB = 8
LANES = 128


def capacity_of(top_k, tokens, experts, tp_size):
    divisor = 32 * experts * tp_size
    return 8 * tp_size * ((5 * top_k * tokens + divisor - 1) // divisor)


def my_coords():
    me = lax.axis_index("ep")
    return me % SIDE, (me // SIDE) % SIDE, me // (SIDE * SIDE)


def iota(shape, dim):
    return lax.broadcasted_iota(jnp.int32, shape, dim)


def route_kernel(cap, units, idx_ref, place_ref, table_ref, hits):
    blocks = idx_ref.shape[0]
    half = cap // 2
    expert_ids = iota((CHIPS, LANES), 0)
    for blk in range(blocks):
        hit = idx_ref[blk:blk + 1, :] == expert_ids
        hits[blk * CHIPS:(blk + 1) * CHIPS, :] = jnp.where(hit, 1.0, 0.0).astype(jnp.bfloat16)
    before = jnp.where(iota((LANES, LANES), 0) < iota((LANES, LANES), 1), 1.0, 0.0)
    mix = jnp.concatenate([before, jnp.ones((LANES, LANES), jnp.float32)], axis=1).astype(jnp.bfloat16)
    counts = jnp.dot(hits[...], mix, preferred_element_type=jnp.float32)
    base = jnp.zeros((CHIPS, LANES), jnp.float32)
    x, y, z = my_coords()
    high = jnp.zeros((CHIPS, cap), jnp.float32)
    low = jnp.zeros((CHIPS, cap), jnp.float32)
    slot_ids = iota((cap, LANES), 0)
    dims = (((1,), (1,)), ((), ()))
    for blk in range(blocks):
        rows = slice(blk * CHIPS, (blk + 1) * CHIPS)
        hit_b = hits[rows, :]
        rank = counts[rows, :LANES] + base
        slot_f = jnp.sum(hit_b.astype(jnp.float32) * rank, axis=0, keepdims=True)
        base = base + counts[rows, LANES:]
        slot = slot_f.astype(jnp.int32)
        tok = iota((1, LANES), 1) + blk * LANES
        match = slot == slot_ids
        tok_hi = (tok // CHIPS).astype(jnp.float32)
        tok_lo = (tok % CHIPS).astype(jnp.float32)
        high = high + lax.dot_general(hit_b, jnp.where(match, tok_hi, 0.0).astype(jnp.bfloat16), dims, preferred_element_type=jnp.float32)
        low = low + lax.dot_general(hit_b, jnp.where(match, tok_lo, 0.0).astype(jnp.bfloat16), dims, preferred_element_type=jnp.float32)
        e = idx_ref[blk:blk + 1, :]
        dx = ((e & 3) - x) & 3
        dy = (((e >> 2) & 3) - y) & 3
        dz = ((e >> 4) - z) & 3
        side = jnp.where(slot >= half, 1, 0)
        rest = slot - side * half
        unit = rest >> 3
        turn = unit + 2 * side
        turn = turn - jnp.where(turn >= 3, 3, 0) - jnp.where(turn >= 6, 3, 0)
        block = jnp.where(turn == 0, dx * 16 + dy * 4 + dz, jnp.where(turn == 1, dy * 16 + dz * 4 + dx, dz * 16 + dx * 4 + dy))
        place = side * (units * CHIPS * SUB) + unit * (CHIPS * SUB) + block * SUB + (rest & 7)
        place_ref[blk:blk + 1, :] = jnp.where(slot < cap, place, CHIPS * cap)
    table_ref[:, :cap] = (high * CHIPS + low).astype(jnp.int32)


def unit_axes(unit, tp):
    x, y, z = my_coords()
    pairs = ((x, 1), (y, SIDE), (z, SIDE * SIDE))
    out = []
    for k in range(3):
        (c0, s0), (c1, s1) = pairs[(unit + k) % 3], pairs[(unit + 2 + k) % 3]
        out.append((c0 * (1 - tp) + c1 * tp, s0 * (1 - tp) + s1 * tp))
    return out


def spread(x_ref, x3, row0, groups):
    cols = x_ref.shape[-1] // LANES

    def step(g, carry):
        v = x_ref[pl.ds(pl.multiple_of(row0 + g * 16, 16), 16), :].astype(jnp.float32)
        at = (row0 + g * 16) * SUB
        for h in range(2):
            for j in range(cols):
                x3[pl.ds(at + h * SUB * SUB + j, SUB, stride=SUB), :] = v[h * SUB:(h + 1) * SUB, j * LANES:(j + 1) * LANES]
        return carry

    lax.fori_loop(0, groups, step, 0, unroll=2)


def gather_kernel(cap, units, table, act, out, stage, x3, tmp, rows_out, in_sem, out_sem):
    tp = lax.axis_index("tp")
    tokens, hidden = act.shape
    cols = hidden // LANES
    chunk = 512
    n = tokens // chunk
    loads = [pltpu.make_async_copy(act.at[pl.ds(k * chunk, chunk)], stage.at[pl.ds(k * chunk, chunk)], in_sem.at[k]) for k in range(n)]
    for c in loads:
        c.start()
    for k in range(n):
        loads[k].wait()
        spread(stage, x3, k * chunk, chunk // 16)
    stores = []
    for u in range(units):
        (a, sa), (b, sb), (c, sc) = unit_axes(u, tp)

        def step(d, carry):
            e = ((a + d // 16) % SIDE) * sa + ((b + (d // 4) % SIDE) % SIDE) * sb + ((c + d % SIDE) % SIDE) * sc
            at = e * cap + tp * (cap // 2) + u * SUB
            for k in range(SUB):
                i = table[at + k]
                tmp[k * SUB:(k + 1) * SUB, :] = x3[pl.ds(pl.multiple_of(i * SUB, SUB), SUB), :]
            for j in range(cols):
                rows_out[u, d, :, j * LANES:(j + 1) * LANES] = tmp[pl.ds(j, SUB, stride=SUB), :].astype(jnp.bfloat16)
            return carry

        lax.fori_loop(0, CHIPS, step, 0)
        st = pltpu.make_async_copy(rows_out.at[u], out.at[u], out_sem.at[u])
        st.start()
        stores.append(st)
    for st in stores:
        st.wait()


def expert_kernel(units, sent, w_in, w_out, out, b1, b2, b3, r1, r2, own, wi, wo, xb, acc, s_sem, r_sem, w_s, w_r, w_l, l_sem, f_s, f_r, f_l):
    tp = lax.axis_index("tp")
    me = lax.axis_index("ep")
    hidden = xb.shape[1]
    halves = w_in.shape[2] // wi.shape[2]
    width = wi.shape[2]

    def dev(ep, core):
        return (0, core, ep)

    def peer(axis, shift):
        pos, stride = axis
        return dev(me + ((pos + shift) % SIDE - pos) * stride, tp)

    axes = [unit_axes(u, tp) for u in range(units)]
    barrier = pltpu.get_barrier_semaphore()
    for axis in axes[0]:
        for shift in (1, 2, 3):
            pl.semaphore_signal(barrier, inc=1, device_id=peer(axis, shift), device_id_type=MESH)
    pl.semaphore_signal(barrier, inc=1, device_id=dev(me, 1 - tp), device_id_type=MESH)
    pl.semaphore_wait(barrier, 10)

    started = []

    def push(src, dst, send, recv, to):
        copy = pltpu.make_async_remote_copy(src_ref=src, dst_ref=dst, send_sem=send, recv_sem=recv, device_id=to, device_id_type=MESH)
        copy.start()
        started.append(copy)
        return copy

    flights = {}

    def leg(phase, u, axis, sign, src_of, dst_of):
        flights[phase, u] = [
            push(src_of(d), dst_of(d), s_sem.at[phase, u, d - 1], r_sem.at[phase, u, d - 1], peer(axis, sign * d)) for d in (1, 2, 3)
        ]

    def landed(phase, u):
        for copy in flights[phase, u]:
            copy.wait_recv()

    locals_ = [pltpu.make_async_copy(sent.at[u, 0], b1.at[u, 0], l_sem.at[u]) for u in range(units)]

    def d1(u):
        locals_[u].start()
        leg(0, u, axes[u][0], 1, lambda d: sent.at[u, d], lambda d: b1.at[u, d])

    def d2(u):
        locals_[u].wait()
        landed(0, u)
        leg(1, u, axes[u][1], 1, lambda d: b1.at[u, :, d], lambda d: b2.at[u, d])
        b2[u, 0] = b1[u, :, 0]

    def d3(u):
        landed(1, u)
        leg(2, u, axes[u][2], 1, lambda d: b2.at[u, :, :, d], lambda d: b3.at[u, d])
        b3[u, 0] = b2[u, :, :, 0]

    def ffn(u):
        landed(2, u)
        for d in range(SIDE):
            v = b3[u, d].astype(jnp.float32).reshape(SIDE * SIDE * SUB, hidden)
            xb[d * SIDE * SIDE * SUB:(d + 1) * SIDE * SIDE * SUB, :] = v.astype(jnp.bfloat16)

        def step(n, carry):
            pre = jnp.dot(xb[...], wi[n], preferred_element_type=jnp.float32)
            mid = jax.nn.gelu(pre, approximate=True).astype(jnp.bfloat16)
            acc[...] += jnp.dot(mid, wo[n], preferred_element_type=jnp.float32)
            return carry

        acc[...] = jnp.zeros_like(acc)
        lax.fori_loop(0, wi.shape[0], step, 0)
        for d in range(SIDE):
            v = acc[d * SIDE * SIDE * SUB:(d + 1) * SIDE * SIDE * SUB, :]
            b3[u, d] = v.reshape(SIDE, SIDE, SUB, hidden).astype(jnp.bfloat16)

    def q1(u):
        leg(3, u, axes[u][2], -1, lambda d: b3.at[u, d], lambda d: r1.at[u, d])
        r1[u, 0] = b3[u, 0]

    def q2(u):
        landed(3, u)
        leg(4, u, axes[u][1], -1, lambda d: r1.at[u, :, d], lambda d: r2.at[u, d])
        r2[u, 0] = r1[u, :, 0]

    def q3(u):
        landed(4, u)
        leg(5, u, axes[u][0], -1, lambda d: r2.at[u, :, :, d], lambda d: own.at[u, d])
        own[u, 0] = r2[u, :, :, 0]

    finals = []

    def fin(u):
        landed(5, u)
        keep = pltpu.make_async_copy(own.at[u], out.at[tp, u], f_l.at[u])
        keep.start()
        finals.append(keep)
        flights["fin", u] = [push(own.at[u], out.at[tp, u], f_s.at[u], f_r.at[u], dev(me, 1 - tp))]

    weights = []
    for j in range(halves):
        n = tp * halves + j
        for k, (src, dst) in enumerate(((w_in.at[0, :, pl.ds(j * width, width)], wi.at[n]), (w_out.at[0, pl.ds(j * width, width), :], wo.at[n]))):
            copy = pltpu.make_async_copy(src, dst, w_l.at[k, j])
            copy.start()
            weights.append(copy)
            flights["w", k, j] = [push(src, dst, w_s.at[k, j], w_r.at[k, j], dev(me, 1 - tp))]

    for u in (0, 1, 2):
        d1(u)
    for u in (0, 1, 2):
        d2(u)
    for u in (3, 4):
        d1(u)
    for u in (0, 1, 2):
        d3(u)
    for u in (3, 4):
        d2(u)
    for copy in weights:
        copy.wait()
    for k in range(2):
        for j in range(halves):
            for copy in flights["w", k, j]:
                copy.wait_recv()
    ffn(0)
    q1(0)
    for u in (3, 4):
        d3(u)
    ffn(1)
    q1(1)
    ffn(2)
    q1(2)
    q2(0)
    ffn(3)
    q1(3)
    q2(1)
    q3(0)
    ffn(4)
    q1(4)
    q2(2)
    q3(1)
    fin(0)
    q2(3)
    q3(2)
    fin(1)
    q2(4)
    q3(3)
    fin(2)
    q3(4)
    fin(3)
    fin(4)
    for u in range(units):
        for copy in flights["fin", u]:
            copy.wait_recv()
    for copy in finals:
        copy.wait()
    for copy in started:
        copy.wait_send()


def combine_kernel(place, gates, rows, out, stage, x3, tmp, rows_out, in_sem, out_sem):
    total, hidden = rows.shape
    tokens = out.shape[0]
    cols = hidden // LANES
    chunk = 512
    n = total // chunk
    loads = [pltpu.make_async_copy(rows.at[pl.ds(k * chunk, chunk)], stage.at[pl.ds(k * chunk, chunk)], in_sem.at[k]) for k in range(n)]
    for c in loads:
        c.start()
    x3[pl.ds(total * SUB, SUB), :] = jnp.zeros((SUB, LANES), jnp.float32)
    for k in range(n):
        loads[k].wait()
        spread(stage, x3, k * chunk, chunk // 16)
    stores = []
    for c in range(tokens // chunk):

        def step(g, carry):
            t0 = c * chunk + g * 16
            for k in range(16):
                i = place[t0 + k]
                tmp[k * SUB:(k + 1) * SUB, :] = x3[pl.ds(pl.multiple_of(i * SUB, SUB), SUB), :] * gates[t0 + k]
            for j in range(cols):
                top = tmp[pl.ds(j, SUB, stride=SUB), :]
                low = tmp[pl.ds(SUB * SUB + j, SUB, stride=SUB), :]
                rows_out[pl.ds(pl.multiple_of(t0, 16), 16), j * LANES:(j + 1) * LANES] = jnp.concatenate([top, low], axis=0).astype(jnp.bfloat16)
            return carry

        lax.fori_loop(0, chunk // 16, step, 0)
        st = pltpu.make_async_copy(rows_out.at[pl.ds(c * chunk, chunk)], out.at[pl.ds(c * chunk, chunk)], out_sem.at[c])
        st.start()
        stores.append(st)
    for st in stores:
        st.wait()


def solution(mesh):
    tp_size = mesh.shape["tp"]
    vmem = pl.BlockSpec(memory_space=pltpu.VMEM)
    smem = pl.BlockSpec(memory_space=pltpu.SMEM)
    hbm = pl.BlockSpec(memory_space=pl.ANY)
    dma = pltpu.SemaphoreType.DMA

    def local_moe(act_loc, idx_loc, gate_loc, w_in, w_out):
        tokens, hidden = act_loc.shape
        cap = capacity_of(1, tokens, CHIPS, tp_size)
        units = cap // tp_size // SUB
        bf16, f32 = jnp.bfloat16, jnp.float32
        place, table = pl.pallas_call(
            functools.partial(route_kernel, cap, units),
            out_shape=(jax.ShapeDtypeStruct((tokens // LANES, LANES), jnp.int32), jax.ShapeDtypeStruct((CHIPS, cap), jnp.int32)),
            in_specs=[vmem],
            out_specs=(vmem, vmem),
            scratch_shapes=[pltpu.VMEM((tokens // LANES * CHIPS, LANES), bf16)],
            name="route",
        )(idx_loc.reshape(tokens // LANES, LANES))
        sent = pl.pallas_call(
            functools.partial(gather_kernel, cap, units),
            out_shape=jax.ShapeDtypeStruct((units, CHIPS, SUB, hidden), bf16),
            in_specs=[smem, hbm],
            out_specs=hbm,
            scratch_shapes=[
                pltpu.VMEM((tokens, hidden), bf16),
                pltpu.VMEM((tokens * SUB, LANES), f32),
                pltpu.VMEM((SUB * SUB, LANES), f32),
                pltpu.VMEM((units, CHIPS, SUB, hidden), bf16),
                dma((8,)),
                dma((units,)),
            ],
            compiler_params=pltpu.CompilerParams(vmem_limit_bytes=48 << 20),
            name="pick",
        )(table.reshape(-1), act_loc)
        cube = (units, SIDE, SIDE, SIDE, SUB, hidden)
        width = 512
        parts = tp_size * w_in.shape[2] // width
        block_rows = CHIPS * SUB
        returned = pl.pallas_call(
            functools.partial(expert_kernel, units),
            out_shape=jax.ShapeDtypeStruct((tp_size,) + cube, bf16),
            in_specs=[hbm, hbm, hbm],
            out_specs=hbm,
            scratch_shapes=[pltpu.VMEM(cube, bf16)] * 6
            + [
                pltpu.VMEM((parts, hidden, width), bf16),
                pltpu.VMEM((parts, width, hidden), bf16),
                pltpu.VMEM((block_rows, hidden), bf16),
                pltpu.VMEM((block_rows, hidden), f32),
                dma((6, units, 3)),
                dma((6, units, 3)),
                dma((2, parts // tp_size)),
                dma((2, parts // tp_size)),
                dma((2, parts // tp_size)),
                dma((units,)),
                dma((units,)),
                dma((units,)),
                dma((units,)),
            ],
            compiler_params=pltpu.CompilerParams(collective_id=0, has_side_effects=True, vmem_limit_bytes=62 << 20),
            name="expert",
        )(sent.reshape(cube), w_in, w_out)
        total = tp_size * units * block_rows
        return pl.pallas_call(
            combine_kernel,
            out_shape=jax.ShapeDtypeStruct((tokens, hidden), bf16),
            in_specs=[smem, smem, hbm],
            out_specs=hbm,
            scratch_shapes=[
                pltpu.VMEM((total, hidden), bf16),
                pltpu.VMEM(((total + 1) * SUB, LANES), f32),
                pltpu.VMEM((2 * SUB * SUB, LANES), f32),
                pltpu.VMEM((tokens, hidden), bf16),
                dma((total // 512,)),
                dma((tokens // 512,)),
            ],
            compiler_params=pltpu.CompilerParams(vmem_limit_bytes=48 << 20),
            name="combine",
        )(place.reshape(-1), gate_loc.reshape(-1), returned.reshape(total, hidden))

    tok_spec = P(("dp", "ep"), None)
    return jax.shard_map(local_moe, mesh=mesh, in_specs=(tok_spec, tok_spec, tok_spec, P("ep", None, "tp"), P("ep", "tp", None)), out_specs=tok_spec, check_vma=False)
```

```python
import functools

import jax
import jax.numpy as jnp
from jax import lax
from jax.experimental import pallas as pl
from jax.experimental.pallas import tpu as pltpu
from jax.sharding import PartitionSpec as P

MESH = pl.DeviceIdType.MESH
SIDE = 4
CHIPS = SIDE ** 3
SUB = 8
LANES = 128
PITCH = 6
ORDER = "a0 a2 a4 a1 b0 a3 b1 c0 b3 b2 w b4 c1 g0 c2 h0 x0 g1 c4 c3 h1 y0 x1 g2 h2 g3 x2 z0 y1 h3 g4 x3 h4 x4 z1 y3 y2 y4 z2 z4 z3 e2 e0 e1 e3 e4"


def capacity_of(top_k, tokens, experts, tp_size):
    divisor = 32 * experts * tp_size
    return 8 * tp_size * ((5 * top_k * tokens + divisor - 1) // divisor)


def my_coords():
    me = lax.axis_index("ep")
    return me % SIDE, (me // SIDE) % SIDE, me // (SIDE * SIDE)


def iota(shape, dim):
    return lax.broadcasted_iota(jnp.int32, shape, dim)


def route_kernel(cap, units, idx_ref, place_ref, table_ref, hits):
    blocks = idx_ref.shape[0]
    half = cap // 2
    expert_ids = iota((CHIPS, LANES), 0)
    for blk in range(blocks):
        hit = idx_ref[blk:blk + 1, :] == expert_ids
        hits[blk * CHIPS:(blk + 1) * CHIPS, :] = jnp.where(hit, 1.0, 0.0).astype(jnp.bfloat16)
    before = jnp.where(iota((LANES, LANES), 0) < iota((LANES, LANES), 1), 1.0, 0.0)
    mix = jnp.concatenate([before, jnp.ones((LANES, LANES), jnp.float32)], axis=1).astype(jnp.bfloat16)
    counts = jnp.dot(hits[...], mix, preferred_element_type=jnp.float32)
    base = jnp.zeros((CHIPS, LANES), jnp.float32)
    x, y, z = my_coords()
    high = jnp.zeros((CHIPS, cap), jnp.float32)
    low = jnp.zeros((CHIPS, cap), jnp.float32)
    slot_ids = iota((cap, LANES), 0)
    dims = (((1,), (1,)), ((), ()))
    for blk in range(blocks):
        rows = slice(blk * CHIPS, (blk + 1) * CHIPS)
        hit_b = hits[rows, :]
        rank = counts[rows, :LANES] + base
        slot_f = jnp.sum(hit_b.astype(jnp.float32) * rank, axis=0, keepdims=True)
        base = base + counts[rows, LANES:]
        slot = slot_f.astype(jnp.int32)
        tok = iota((1, LANES), 1) + blk * LANES
        match = slot == slot_ids
        tok_hi = (tok // CHIPS).astype(jnp.float32)
        tok_lo = (tok % CHIPS).astype(jnp.float32)
        high = high + lax.dot_general(hit_b, jnp.where(match, tok_hi, 0.0).astype(jnp.bfloat16), dims, preferred_element_type=jnp.float32)
        low = low + lax.dot_general(hit_b, jnp.where(match, tok_lo, 0.0).astype(jnp.bfloat16), dims, preferred_element_type=jnp.float32)
        e = idx_ref[blk:blk + 1, :]
        dx = ((e & 3) - x) & 3
        dy = (((e >> 2) & 3) - y) & 3
        dz = ((e >> 4) - z) & 3
        side = jnp.where(slot >= half, 1, 0)
        rest = slot - side * half
        unit = rest >> 3
        turn = unit + 2 * side
        turn = turn - jnp.where(turn >= 3, 3, 0) - jnp.where(turn >= 6, 3, 0)
        block = jnp.where(turn == 0, dx * 16 + dy * 4 + dz, jnp.where(turn == 1, dy * 16 + dz * 4 + dx, dz * 16 + dx * 4 + dy))
        place = side * (units * CHIPS * SUB) + unit * (CHIPS * SUB) + block * SUB + (rest & 7)
        place_ref[blk:blk + 1, :] = jnp.where(slot < cap, place, CHIPS * cap) * PITCH
    table_ref[...] = (high * CHIPS + low).astype(jnp.int32) * PITCH


def unit_axes(unit, tp):
    x, y, z = my_coords()
    pairs = ((x, 1), (y, SIDE), (z, SIDE * SIDE))
    out = []
    for k in range(3):
        (c0, s0), (c1, s1) = pairs[(unit + k) % 3], pairs[(unit + 2 + k) % 3]
        out.append((c0 * (1 - tp) + c1 * tp, s0 * (1 - tp) + s1 * tp))
    return out


def spread(x_ref, x3, src0, dst0, groups):
    cols = x_ref.shape[-1] // LANES

    def step(g, carry):
        v = x_ref[pl.ds(pl.multiple_of(src0 + g * 16, 16), 16), :].astype(jnp.float32)
        at = (dst0 + g * 16) * PITCH
        for h in range(2):
            for j in range(cols):
                x3[pl.ds(at + h * SUB * PITCH + j, SUB, stride=PITCH), :] = v[h * SUB:(h + 1) * SUB, j * LANES:(j + 1) * LANES]
        return carry

    lax.fori_loop(0, groups, step, 0, unroll=4)


def expert_kernel(cap, units, table, act, w_in, w_out, out, stage, x3, tmp, sent, b1, b2, b3, r1, r2, own, wi, wo, xb, acc, a_sem, s_sem, r_sem, w_s, w_r, w_l, f_s, f_r, f_l):
    tp = lax.axis_index("tp")
    me = lax.axis_index("ep")
    hidden = xb.shape[1]
    cols = hidden // LANES
    slots, chunk = stage.shape[:2]
    pieces = act.shape[0] // chunk
    tall = SIDE * SIDE * SUB
    loads = [pltpu.make_async_copy(act.at[pl.ds(k * chunk, chunk)], stage.at[k % slots], a_sem.at[k]) for k in range(pieces)]
    for copy in loads[:slots]:
        copy.start()

    def dev(ep, core):
        return (0, core, ep)

    def peer(axis, shift):
        pos, stride = axis
        return dev(me + ((pos + shift) % SIDE - pos) * stride, tp)

    axes = [unit_axes(u, tp) for u in range(units)]
    barrier = pltpu.get_barrier_semaphore()
    for axis in axes[0]:
        for shift in (1, 2, 3):
            pl.semaphore_signal(barrier, inc=1, device_id=peer(axis, shift), device_id_type=MESH)
    pl.semaphore_signal(barrier, inc=1, device_id=dev(me, 1 - tp), device_id_type=MESH)
    for k in range(pieces):
        loads[k].wait()
        spread(stage.at[k % slots], x3, 0, k * chunk, chunk // 16)
        if k + slots < pieces:
            loads[k + slots].start()
    pl.semaphore_wait(barrier, 10)

    started = []

    def push(src, dst, send, recv, to):
        copy = pltpu.make_async_remote_copy(src_ref=src, dst_ref=dst, send_sem=send, recv_sem=recv, device_id=to, device_id_type=MESH)
        copy.start()
        started.append(copy)
        return copy

    flights = {}

    def leg(phase, u, axis, sign, src_of, dst_of):
        flights[phase, u] = [
            push(src_of(d), dst_of(d), s_sem.at[phase, u, d - 1], r_sem.at[phase, u, d - 1], peer(axis, sign * d)) for d in (1, 2, 3)
        ]

    def landed(phase, u):
        for copy in flights[phase, u]:
            copy.wait_recv()

    def pick(u, shift, target):
        (a, sa), (b, sb), (c, sc) = axes[u]

        def step(db, carry):
            rows = []
            for dc in range(SIDE):
                e = ((a + shift) % SIDE) * sa + ((b + db) % SIDE) * sb + ((c + dc) % SIDE) * sc
                at = tp * (cap // 2) + u * SUB
                rows += [x3[pl.ds(table[e, at + k], SUB), :] for k in range(SUB)]
            for k, row in enumerate(rows):
                tmp[k * SUB:(k + 1) * SUB, :] = row
            for dc in range(SIDE):
                for j in range(cols):
                    target[db, dc, :, j * LANES:(j + 1) * LANES] = tmp[pl.ds(dc * SUB * SUB + j, SUB, stride=SUB), :].astype(jnp.bfloat16)
            return carry

        lax.fori_loop(0, SIDE, step, 0, unroll=2)

    def d1(u):
        for shift in range(1, SIDE):
            pick(u, shift, sent.at[u, shift - 1])
        leg(0, u, axes[u][0], 1, lambda d: sent.at[u, d - 1], lambda d: b1.at[u, d])
        pick(u, 0, b1.at[u, 0])

    def d2(u):
        landed(0, u)
        leg(1, u, axes[u][1], 1, lambda d: b1.at[u, :, d], lambda d: b2.at[u, d])
        b2[u, 0] = b1[u, :, 0]

    def d3(u):
        landed(1, u)
        leg(2, u, axes[u][2], 1, lambda d: b2.at[u, :, :, d], lambda d: b3.at[u, d])
        b3[u, 0] = b2[u, :, :, 0]

    def half(u, n, d):
        rows = slice(d * tall, (d + 1) * tall)
        pre = jnp.dot(xb[rows, :], wi[n], preferred_element_type=jnp.float32)
        mid = jax.nn.gelu(pre, approximate=True).astype(jnp.bfloat16)
        return jnp.dot(mid, wo[n], preferred_element_type=jnp.float32)

    def first(u):
        landed(2, u)
        for d in range(SIDE):
            rows = slice(d * tall, (d + 1) * tall)
            xb[rows, :] = b3[u, d].astype(jnp.float32).reshape(tall, hidden).astype(jnp.bfloat16)
        for d in range(SIDE):
            acc[d * tall:(d + 1) * tall, :] = half(u, 0, d)

    def second(u):
        for d in range(SIDE):
            total = acc[d * tall:(d + 1) * tall, :] + half(u, 1, d)
            b3[u, d] = total.reshape(SIDE, SIDE, SUB, hidden).astype(jnp.bfloat16)

    def q1(u):
        leg(3, u, axes[u][2], -1, lambda d: b3.at[u, d], lambda d: r1.at[u, d])
        r1[u, 0] = b3[u, 0]

    def q2(u):
        landed(3, u)
        leg(4, u, axes[u][1], -1, lambda d: r1.at[u, :, d], lambda d: r2.at[u, d])
        r2[u, 0] = r1[u, :, 0]

    def q3(u):
        landed(4, u)
        leg(5, u, axes[u][0], -1, lambda d: r2.at[u, :, :, d], lambda d: own.at[u, d])
        own[u, 0] = r2[u, :, :, 0]

    finals = []

    def fin(u):
        landed(5, u)
        keep = pltpu.make_async_copy(own.at[u], out.at[tp, u], f_l.at[u])
        keep.start()
        finals.append(keep)
        flights["fin", u] = [push(own.at[u], out.at[tp, u], f_s.at[u], f_r.at[u], dev(me, 1 - tp))]

    weights = []
    for k, (src, dst) in enumerate(((w_in.at[0], wi.at[tp]), (w_out.at[0], wo.at[tp]))):
        copy = pltpu.make_async_copy(src, dst, w_l.at[k])
        copy.start()
        weights.append(copy)
        flights["w", k] = [push(src, dst, w_s.at[k], w_r.at[k], dev(me, 1 - tp))]

    def ready():
        for copy in weights:
            copy.wait()
        for k in range(2):
            for copy in flights["w", k]:
                copy.wait_recv()

    ops = {"a": d1, "b": d2, "c": d3, "g": first, "h": second, "x": q1, "y": q2, "z": q3, "e": fin}
    for word in ORDER.split():
        if word == "w":
            ready()
        else:
            ops[word[0]](int(word[1]))
    for u in range(units):
        for copy in flights["fin", u]:
            copy.wait_recv()
    for copy in finals:
        copy.wait()
    for copy in started:
        copy.wait_send()


def combine_kernel(place, gates, rows, out, stage, x3, tmp, scale, rows_out, in_sem, out_sem):
    total, hidden = rows.shape
    tokens = out.shape[0]
    cols = hidden // LANES
    chunk = 512
    n = total // chunk
    loads = [pltpu.make_async_copy(rows.at[pl.ds(k * chunk, chunk)], stage.at[pl.ds(k * chunk, chunk)], in_sem.at[k]) for k in range(n)]
    for c in loads:
        c.start()
    x3[pl.ds(total * PITCH, SUB), :] = jnp.zeros((SUB, LANES), jnp.float32)
    for k in range(tokens // LANES):
        scale[k * LANES:(k + 1) * LANES, :] = jnp.transpose(jnp.broadcast_to(gates[k:k + 1, :], (LANES, LANES)))
    for k in range(n):
        loads[k].wait()
        spread(stage, x3, k * chunk, k * chunk, chunk // 16)
    stores = []
    for c in range(tokens // chunk):

        def step(g, carry):
            t0 = c * chunk + g * 32
            picked = [x3[pl.ds(place[t0 + k], SUB), :] for k in range(32)]
            for k, row in enumerate(picked):
                tmp[k * SUB:(k + 1) * SUB, :] = row
            for h in range(2):
                gate_a = scale[pl.ds(pl.multiple_of(t0 + h * 16, SUB), SUB), :]
                gate_b = scale[pl.ds(pl.multiple_of(t0 + h * 16 + SUB, SUB), SUB), :]
                for j in range(cols):
                    top = tmp[pl.ds(2 * h * SUB * SUB + j, SUB, stride=SUB), :] * gate_a
                    low = tmp[pl.ds((2 * h + 1) * SUB * SUB + j, SUB, stride=SUB), :] * gate_b
                    rows_out[pl.ds(pl.multiple_of(t0 + h * 16, 16), 16), j * LANES:(j + 1) * LANES] = jnp.concatenate([top, low], axis=0).astype(jnp.bfloat16)
            return carry

        lax.fori_loop(0, chunk // 32, step, 0, unroll=2)
        st = pltpu.make_async_copy(rows_out.at[pl.ds(c * chunk, chunk)], out.at[pl.ds(c * chunk, chunk)], out_sem.at[c])
        st.start()
        stores.append(st)
    for st in stores:
        st.wait()


def solution(mesh):
    tp_size = mesh.shape["tp"]
    vmem = pl.BlockSpec(memory_space=pltpu.VMEM)
    smem = pl.BlockSpec(memory_space=pltpu.SMEM)
    hbm = pl.BlockSpec(memory_space=pl.ANY)
    dma = pltpu.SemaphoreType.DMA

    def local_moe(act_loc, idx_loc, gate_loc, w_in, w_out):
        tokens, hidden = act_loc.shape
        cap = capacity_of(1, tokens, CHIPS, tp_size)
        units = cap // tp_size // SUB
        bf16, f32 = jnp.bfloat16, jnp.float32
        place, table = pl.pallas_call(
            functools.partial(route_kernel, cap, units),
            out_shape=(jax.ShapeDtypeStruct((tokens // LANES, LANES), jnp.int32), jax.ShapeDtypeStruct((CHIPS, cap), jnp.int32)),
            in_specs=[vmem],
            out_specs=(vmem, vmem),
            scratch_shapes=[pltpu.VMEM((tokens // LANES * CHIPS, LANES), bf16)],
            name="route",
        )(idx_loc.reshape(tokens // LANES, LANES))
        cube = (units, SIDE, SIDE, SIDE, SUB, hidden)
        width = w_in.shape[2]
        block_rows = CHIPS * SUB
        chunk = 512
        returned = pl.pallas_call(
            functools.partial(expert_kernel, cap, units),
            out_shape=jax.ShapeDtypeStruct((tp_size,) + cube, bf16),
            in_specs=[smem, hbm, hbm, hbm],
            out_specs=hbm,
            scratch_shapes=[
                pltpu.VMEM((4, chunk, hidden), bf16),
                pltpu.VMEM((tokens * PITCH + SUB, LANES), f32),
                pltpu.VMEM((SIDE * SUB * SUB, LANES), f32),
                pltpu.VMEM((units, SIDE - 1) + cube[2:], bf16),
            ]
            + [pltpu.VMEM(cube, bf16)] * 6
            + [
                pltpu.VMEM((tp_size, hidden, width), bf16),
                pltpu.VMEM((tp_size, width, hidden), bf16),
                pltpu.VMEM((block_rows, hidden), bf16),
                pltpu.VMEM((block_rows, hidden), f32),
                dma((tokens // chunk,)),
                dma((6, units, 3)),
                dma((6, units, 3)),
                dma((2,)),
                dma((2,)),
                dma((2,)),
                dma((units,)),
                dma((units,)),
                dma((units,)),
            ],
            compiler_params=pltpu.CompilerParams(collective_id=0, has_side_effects=True, vmem_limit_bytes=67043328),
            name="expert",
        )(table, act_loc, w_in, w_out)
        total = tp_size * units * block_rows
        return pl.pallas_call(
            combine_kernel,
            out_shape=jax.ShapeDtypeStruct((tokens, hidden), bf16),
            in_specs=[smem, vmem, hbm],
            out_specs=hbm,
            scratch_shapes=[
                pltpu.VMEM((total, hidden), bf16),
                pltpu.VMEM((total * PITCH + SUB, LANES), f32),
                pltpu.VMEM((4 * SUB * SUB, LANES), f32),
                pltpu.VMEM((tokens, LANES), f32),
                pltpu.VMEM((tokens, hidden), bf16),
                dma((total // 512,)),
                dma((tokens // 512,)),
            ],
            compiler_params=pltpu.CompilerParams(vmem_limit_bytes=48 << 20),
            name="combine",
        )(place.reshape(-1), gate_loc.reshape(tokens // LANES, LANES), returned.reshape(total, hidden))

    tok_spec = P(("dp", "ep"), None)
    return jax.shard_map(local_moe, mesh=mesh, in_specs=(tok_spec, tok_spec, tok_spec, P("ep", None, "tp"), P("ep", "tp", None)), out_specs=tok_spec, check_vma=False)
```

```python
import functools

import jax
import jax.numpy as jnp
from jax import lax
from jax.experimental import pallas as pl
from jax.experimental.pallas import tpu as pltpu
from jax.sharding import PartitionSpec as P

MESH = pl.DeviceIdType.MESH
SIDE = 4
CHIPS = SIDE ** 3
SUB = 8
LANES = 128
PITCH = 6
ORDER = (
    "a0", "a2", "a1", "a3", "b0", "w", "b2", "b1", "a4", "c0", "c1", "b3",
    "b4", "c2", "g0", "h0", "x0", "g1", "h1", "c3", "x1", "c4", "g2", "y0",
    "h2", "x2", "y1", "g3", "h3", "x3", "z0", "g4", "h4", "x4", "z1", "y4",
    "y2", "y3", "e1", "z4", "z2", "z3", "e2", "e3", "e4", "e0",
)


def capacity_of(top_k, tokens, experts, tp_size):
    divisor = 32 * experts * tp_size
    return 8 * tp_size * ((5 * top_k * tokens + divisor - 1) // divisor)


def my_coords():
    me = lax.axis_index("ep")
    return me % SIDE, (me // SIDE) % SIDE, me // (SIDE * SIDE)


def iota(shape, dim):
    return lax.broadcasted_iota(jnp.int32, shape, dim)


def route_kernel(cap, units, idx_ref, place_ref, table_ref, hits):
    blocks = idx_ref.shape[0]
    half = cap // 2
    expert_ids = iota((CHIPS, LANES), 0)
    for blk in range(blocks):
        hit = idx_ref[blk:blk + 1, :] == expert_ids
        hits[blk * CHIPS:(blk + 1) * CHIPS, :] = jnp.where(hit, 1.0, 0.0).astype(jnp.bfloat16)
    before = jnp.where(iota((LANES, LANES), 0) < iota((LANES, LANES), 1), 1.0, 0.0)
    mix = jnp.concatenate([before, jnp.ones((LANES, LANES), jnp.float32)], axis=1).astype(jnp.bfloat16)
    counts = jnp.dot(hits[...], mix, preferred_element_type=jnp.float32)
    base = jnp.zeros((CHIPS, LANES), jnp.float32)
    x, y, z = my_coords()
    high = jnp.zeros((CHIPS, cap), jnp.float32)
    low = jnp.zeros((CHIPS, cap), jnp.float32)
    slot_ids = iota((cap, LANES), 0)
    dims = (((1,), (1,)), ((), ()))
    for blk in range(blocks):
        rows = slice(blk * CHIPS, (blk + 1) * CHIPS)
        hit_b = hits[rows, :]
        rank = counts[rows, :LANES] + base
        slot_f = jnp.sum(hit_b.astype(jnp.float32) * rank, axis=0, keepdims=True)
        base = base + counts[rows, LANES:]
        slot = slot_f.astype(jnp.int32)
        tok = iota((1, LANES), 1) + blk * LANES
        match = slot == slot_ids
        tok_hi = (tok // CHIPS).astype(jnp.float32)
        tok_lo = (tok % CHIPS).astype(jnp.float32)
        high = high + lax.dot_general(hit_b, jnp.where(match, tok_hi, 0.0).astype(jnp.bfloat16), dims, preferred_element_type=jnp.float32)
        low = low + lax.dot_general(hit_b, jnp.where(match, tok_lo, 0.0).astype(jnp.bfloat16), dims, preferred_element_type=jnp.float32)
        e = idx_ref[blk:blk + 1, :]
        dx = ((e & 3) - x) & 3
        dy = (((e >> 2) & 3) - y) & 3
        dz = ((e >> 4) - z) & 3
        side = jnp.where(slot >= half, 1, 0)
        rest = slot - side * half
        unit = rest >> 3
        turn = unit + 2 * side
        turn = turn - jnp.where(turn >= 3, 3, 0) - jnp.where(turn >= 6, 3, 0)
        block = jnp.where(turn == 0, dx * 16 + dy * 4 + dz, jnp.where(turn == 1, dy * 16 + dz * 4 + dx, dz * 16 + dx * 4 + dy))
        place = side * (units * CHIPS * SUB) + unit * (CHIPS * SUB) + block * SUB + (rest & 7)
        place_ref[blk:blk + 1, :] = jnp.where(slot < cap, place, CHIPS * cap) * PITCH
    table_ref[...] = (high * CHIPS + low).astype(jnp.int32) * PITCH


def unit_axes(unit, tp):
    x, y, z = my_coords()
    pairs = ((x, 1), (y, SIDE), (z, SIDE * SIDE))
    out = []
    for k in range(3):
        (c0, s0), (c1, s1) = pairs[(unit + k) % 3], pairs[(unit + 2 + k) % 3]
        out.append((c0 * (1 - tp) + c1 * tp, s0 * (1 - tp) + s1 * tp))
    return out


def spread(x_ref, x3, src0, dst0, groups):
    cols = x_ref.shape[-1] // LANES

    def step(g, carry):
        v = x_ref[pl.ds(pl.multiple_of(src0 + g * 16, 16), 16), :].astype(jnp.float32)
        at = (dst0 + g * 16) * PITCH
        for h in range(2):
            for j in range(cols):
                x3[pl.ds(at + h * SUB * PITCH + j, SUB, stride=PITCH), :] = v[h * SUB:(h + 1) * SUB, j * LANES:(j + 1) * LANES]
        return carry

    lax.fori_loop(0, groups, step, 0, unroll=4)


def expert_kernel(cap, units, table, act, w_in, w_out, out, stage, x3, tmp, sent, b1, b2, b3, r1, r2, own, wi, wo, xb, acc, a_sem, s_sem, r_sem, w_s, w_r, w_l, f_s, f_r, f_l):
    tp = lax.axis_index("tp")
    me = lax.axis_index("ep")
    hidden = xb.shape[1]
    cols = hidden // LANES
    slots, chunk = stage.shape[:2]
    pieces = act.shape[0] // chunk
    tall = SIDE * SIDE * SUB
    loads = [pltpu.make_async_copy(act.at[pl.ds(k * chunk, chunk)], stage.at[k % slots], a_sem.at[k]) for k in range(pieces)]
    for copy in loads[:slots]:
        copy.start()

    def dev(ep, core):
        return (0, core, ep)

    def peer(axis, shift):
        pos, stride = axis
        return dev(me + ((pos + shift) % SIDE - pos) * stride, tp)

    axes = [unit_axes(u, tp) for u in range(units)]
    barrier = pltpu.get_barrier_semaphore()
    for axis in axes[0]:
        for shift in (1, 2, 3):
            pl.semaphore_signal(barrier, inc=1, device_id=peer(axis, shift), device_id_type=MESH)
    pl.semaphore_signal(barrier, inc=1, device_id=dev(me, 1 - tp), device_id_type=MESH)
    for k in range(pieces):
        loads[k].wait()
        spread(stage.at[k % slots], x3, 0, k * chunk, chunk // 16)
        if k + slots < pieces:
            loads[k + slots].start()
    pl.semaphore_wait(barrier, 10)

    started = []

    def push(src, dst, send, recv, to):
        copy = pltpu.make_async_remote_copy(src_ref=src, dst_ref=dst, send_sem=send, recv_sem=recv, device_id=to, device_id_type=MESH)
        copy.start()
        started.append(copy)
        return copy

    flights = {}

    def leg(phase, u, axis, sign, src_of, dst_of):
        flights[phase, u] = [
            push(src_of(d), dst_of(d), s_sem.at[phase, u, d - 1], r_sem.at[phase, u, d - 1], peer(axis, sign * d)) for d in (1, 2, 3)
        ]

    def landed(phase, u):
        for copy in flights[phase, u]:
            copy.wait_recv()

    def pick(u, shift, target):
        (a, sa), (b, sb), (c, sc) = axes[u]

        def step(db, carry):
            rows = []
            for dc in range(SIDE):
                e = ((a + shift) % SIDE) * sa + ((b + db) % SIDE) * sb + ((c + dc) % SIDE) * sc
                at = tp * (cap // 2) + u * SUB
                rows += [x3[pl.ds(table[e, at + k], SUB), :] for k in range(SUB)]
            for k, row in enumerate(rows):
                tmp[k * SUB:(k + 1) * SUB, :] = row
            for dc in range(SIDE):
                for j in range(cols):
                    target[db, dc, :, j * LANES:(j + 1) * LANES] = tmp[pl.ds(dc * SUB * SUB + j, SUB, stride=SUB), :].astype(jnp.bfloat16)
            return carry

        lax.fori_loop(0, SIDE, step, 0, unroll=2)

    def d1(u):
        for shift in range(1, SIDE):
            pick(u, shift, sent.at[u, shift - 1])
        leg(0, u, axes[u][0], 1, lambda d: sent.at[u, d - 1], lambda d: b1.at[u, d])
        pick(u, 0, b1.at[u, 0])

    def d2(u):
        landed(0, u)
        leg(1, u, axes[u][1], 1, lambda d: b1.at[u, :, d], lambda d: b2.at[u, d])
        b2[u, 0] = b1[u, :, 0]

    def d3(u):
        landed(1, u)
        leg(2, u, axes[u][2], 1, lambda d: b2.at[u, :, :, d], lambda d: b3.at[u, d])
        b3[u, 0] = b2[u, :, :, 0]

    def half(u, n, d):
        rows = slice(d * tall, (d + 1) * tall)
        pre = jnp.dot(xb[rows, :], wi[n], preferred_element_type=jnp.float32)
        mid = jax.nn.gelu(pre, approximate=True).astype(jnp.bfloat16)
        return jnp.dot(mid, wo[n], preferred_element_type=jnp.float32)

    def first(u):
        landed(2, u)
        for d in range(SIDE):
            rows = slice(d * tall, (d + 1) * tall)
            xb[rows, :] = b3[u, d].astype(jnp.float32).reshape(tall, hidden).astype(jnp.bfloat16)
        for d in range(SIDE):
            acc[d * tall:(d + 1) * tall, :] = half(u, 0, d)

    def second(u):
        for d in range(SIDE):
            total = acc[d * tall:(d + 1) * tall, :] + half(u, 1, d)
            b3[u, d] = total.reshape(SIDE, SIDE, SUB, hidden).astype(jnp.bfloat16)

    def q1(u):
        leg(3, u, axes[u][2], -1, lambda d: b3.at[u, d], lambda d: r1.at[u, d])
        r1[u, 0] = b3[u, 0]

    def q2(u):
        landed(3, u)
        leg(4, u, axes[u][1], -1, lambda d: r1.at[u, :, d], lambda d: r2.at[u, d])
        r2[u, 0] = r1[u, :, 0]

    def q3(u):
        landed(4, u)
        leg(5, u, axes[u][0], -1, lambda d: r2.at[u, :, :, d], lambda d: own.at[u, d])
        own[u, 0] = r2[u, :, :, 0]

    finals = []

    def fin(u):
        landed(5, u)
        keep = pltpu.make_async_copy(own.at[u], out.at[tp, u], f_l.at[u])
        keep.start()
        finals.append(keep)
        flights["fin", u] = [push(own.at[u], out.at[tp, u], f_s.at[u], f_r.at[u], dev(me, 1 - tp))]

    weights = []
    for k, (src, dst) in enumerate(((w_in.at[0], wi.at[tp]), (w_out.at[0], wo.at[tp]))):
        copy = pltpu.make_async_copy(src, dst, w_l.at[k])
        copy.start()
        weights.append(copy)
        flights["w", k] = [push(src, dst, w_s.at[k], w_r.at[k], dev(me, 1 - tp))]

    def ready():
        for copy in weights:
            copy.wait()
        for k in range(2):
            for copy in flights["w", k]:
                copy.wait_recv()

    ops = {"a": d1, "b": d2, "c": d3, "g": first, "h": second, "x": q1, "y": q2, "z": q3, "e": fin}
    for word in ORDER:
        if word == "w":
            ready()
        else:
            ops[word[0]](int(word[1]))
    for u in range(units):
        for copy in flights["fin", u]:
            copy.wait_recv()
    for copy in finals:
        copy.wait()
    for copy in started:
        copy.wait_send()


def combine_kernel(place, gates, rows, out, stage, x3, tmp, scale, rows_out, in_sem, out_sem):
    total, hidden = rows.shape
    tokens = out.shape[0]
    cols = hidden // LANES
    chunk = 512
    n = total // chunk
    loads = [pltpu.make_async_copy(rows.at[pl.ds(k * chunk, chunk)], stage.at[pl.ds(k * chunk, chunk)], in_sem.at[k]) for k in range(n)]
    for c in loads:
        c.start()
    x3[pl.ds(total * PITCH, SUB), :] = jnp.zeros((SUB, LANES), jnp.float32)
    for k in range(tokens // LANES):
        scale[k * LANES:(k + 1) * LANES, :] = jnp.transpose(jnp.broadcast_to(gates[k:k + 1, :], (LANES, LANES)))
    for k in range(n):
        loads[k].wait()
        spread(stage, x3, k * chunk, k * chunk, chunk // 16)
    stores = []
    for c in range(tokens // chunk):

        def step(g, carry):
            t0 = c * chunk + g * 32
            picked = [x3[pl.ds(place[t0 + k], SUB), :] for k in range(32)]
            for k, row in enumerate(picked):
                tmp[k * SUB:(k + 1) * SUB, :] = row
            for h in range(2):
                gate_a = scale[pl.ds(pl.multiple_of(t0 + h * 16, SUB), SUB), :]
                gate_b = scale[pl.ds(pl.multiple_of(t0 + h * 16 + SUB, SUB), SUB), :]
                for j in range(cols):
                    top = tmp[pl.ds(2 * h * SUB * SUB + j, SUB, stride=SUB), :] * gate_a
                    low = tmp[pl.ds((2 * h + 1) * SUB * SUB + j, SUB, stride=SUB), :] * gate_b
                    rows_out[pl.ds(pl.multiple_of(t0 + h * 16, 16), 16), j * LANES:(j + 1) * LANES] = jnp.concatenate([top, low], axis=0).astype(jnp.bfloat16)
            return carry

        lax.fori_loop(0, chunk // 32, step, 0, unroll=2)
        st = pltpu.make_async_copy(rows_out.at[pl.ds(c * chunk, chunk)], out.at[pl.ds(c * chunk, chunk)], out_sem.at[c])
        st.start()
        stores.append(st)
    for st in stores:
        st.wait()


def solution(mesh):
    tp_size = mesh.shape["tp"]
    vmem = pl.BlockSpec(memory_space=pltpu.VMEM)
    smem = pl.BlockSpec(memory_space=pltpu.SMEM)
    hbm = pl.BlockSpec(memory_space=pl.ANY)
    dma = pltpu.SemaphoreType.DMA

    def local_moe(act_loc, idx_loc, gate_loc, w_in, w_out):
        tokens, hidden = act_loc.shape
        cap = capacity_of(1, tokens, CHIPS, tp_size)
        units = cap // tp_size // SUB
        bf16, f32 = jnp.bfloat16, jnp.float32
        place, table = pl.pallas_call(
            functools.partial(route_kernel, cap, units),
            out_shape=(jax.ShapeDtypeStruct((tokens // LANES, LANES), jnp.int32), jax.ShapeDtypeStruct((CHIPS, cap), jnp.int32)),
            in_specs=[vmem],
            out_specs=(vmem, vmem),
            scratch_shapes=[pltpu.VMEM((tokens // LANES * CHIPS, LANES), bf16)],
            name="route",
        )(idx_loc.reshape(tokens // LANES, LANES))
        cube = (units, SIDE, SIDE, SIDE, SUB, hidden)
        width = w_in.shape[2]
        block_rows = CHIPS * SUB
        chunk = 512
        returned = pl.pallas_call(
            functools.partial(expert_kernel, cap, units),
            out_shape=jax.ShapeDtypeStruct((tp_size,) + cube, bf16),
            in_specs=[smem, hbm, hbm, hbm],
            out_specs=hbm,
            scratch_shapes=[
                pltpu.VMEM((4, chunk, hidden), bf16),
                pltpu.VMEM((tokens * PITCH + SUB, LANES), f32),
                pltpu.VMEM((SIDE * SUB * SUB, LANES), f32),
                pltpu.VMEM((units, SIDE - 1) + cube[2:], bf16),
            ]
            + [pltpu.VMEM(cube, bf16)] * 6
            + [
                pltpu.VMEM((tp_size, hidden, width), bf16),
                pltpu.VMEM((tp_size, width, hidden), bf16),
                pltpu.VMEM((block_rows, hidden), bf16),
                pltpu.VMEM((block_rows, hidden), f32),
                dma((tokens // chunk,)),
                dma((6, units, 3)),
                dma((6, units, 3)),
                dma((2,)),
                dma((2,)),
                dma((2,)),
                dma((units,)),
                dma((units,)),
                dma((units,)),
            ],
            compiler_params=pltpu.CompilerParams(collective_id=0, has_side_effects=True, vmem_limit_bytes=67043328),
            name="expert",
        )(table, act_loc, w_in, w_out)
        total = tp_size * units * block_rows
        return pl.pallas_call(
            combine_kernel,
            out_shape=jax.ShapeDtypeStruct((tokens, hidden), bf16),
            in_specs=[smem, vmem, hbm],
            out_specs=hbm,
            scratch_shapes=[
                pltpu.VMEM((total, hidden), bf16),
                pltpu.VMEM((total * PITCH + SUB, LANES), f32),
                pltpu.VMEM((4 * SUB * SUB, LANES), f32),
                pltpu.VMEM((tokens, LANES), f32),
                pltpu.VMEM((tokens, hidden), bf16),
                dma((total // 512,)),
                dma((tokens // 512,)),
            ],
            compiler_params=pltpu.CompilerParams(vmem_limit_bytes=48 << 20),
            name="combine",
        )(place.reshape(-1), gate_loc.reshape(tokens // LANES, LANES), returned.reshape(total, hidden))

    tok_spec = P(("dp", "ep"), None)
    return jax.shard_map(local_moe, mesh=mesh, in_specs=(tok_spec, tok_spec, tok_spec, P("ep", None, "tp"), P("ep", "tp", None)), out_specs=tok_spec, check_vma=False)
```

```python
import functools

import jax
import jax.numpy as jnp
from jax import lax
from jax.experimental import pallas as pl
from jax.experimental.pallas import tpu as pltpu
from jax.sharding import PartitionSpec as P

MESH = pl.DeviceIdType.MESH
SIDE = 4
CHIPS = SIDE ** 3
SUB = 8
LANES = 128
PITCH = 6
ORDER = (
    "a0", "a2", "a1", "a3", "b0", "w", "b2", "b1", "a4", "c0", "c1", "b3",
    "b4", "c2", "g0", "h0", "x0", "g1", "h1", "c3", "x1", "c4", "g2", "y0",
    "h2", "x2", "y1", "g3", "h3", "x3", "z0", "g4", "h4", "x4", "z1", "y4",
    "y2", "y3", "e1", "z4", "z2", "z3", "e2", "e3", "e4", "e0",
)


def capacity_of(top_k, tokens, experts, tp_size):
    divisor = 32 * experts * tp_size
    return 8 * tp_size * ((5 * top_k * tokens + divisor - 1) // divisor)


def my_coords():
    me = lax.axis_index("ep")
    return me % SIDE, (me // SIDE) % SIDE, me // (SIDE * SIDE)


def iota(shape, dim):
    return lax.broadcasted_iota(jnp.int32, shape, dim)


def route_kernel(cap, units, idx_ref, place_ref, table_ref, hits):
    blocks = idx_ref.shape[0]
    half = cap // 2
    expert_ids = iota((CHIPS, LANES), 0)
    for blk in range(blocks):
        hit = idx_ref[blk:blk + 1, :] == expert_ids
        hits[blk * CHIPS:(blk + 1) * CHIPS, :] = jnp.where(hit, 1.0, 0.0).astype(jnp.bfloat16)
    before = jnp.where(iota((LANES, LANES), 0) < iota((LANES, LANES), 1), 1.0, 0.0)
    mix = jnp.concatenate([before, jnp.ones((LANES, LANES), jnp.float32)], axis=1).astype(jnp.bfloat16)
    counts = jnp.dot(hits[...], mix, preferred_element_type=jnp.float32)
    base = jnp.zeros((CHIPS, LANES), jnp.float32)
    x, y, z = my_coords()
    high = jnp.zeros((CHIPS, cap), jnp.float32)
    low = jnp.zeros((CHIPS, cap), jnp.float32)
    slot_ids = iota((cap, LANES), 0)
    dims = (((1,), (1,)), ((), ()))
    for blk in range(blocks):
        rows = slice(blk * CHIPS, (blk + 1) * CHIPS)
        hit_b = hits[rows, :]
        rank = counts[rows, :LANES] + base
        slot_f = jnp.sum(hit_b.astype(jnp.float32) * rank, axis=0, keepdims=True)
        base = base + counts[rows, LANES:]
        slot = slot_f.astype(jnp.int32)
        tok = iota((1, LANES), 1) + blk * LANES
        match = slot == slot_ids
        tok_hi = (tok // CHIPS).astype(jnp.float32)
        tok_lo = (tok % CHIPS).astype(jnp.float32)
        high = high + lax.dot_general(hit_b, jnp.where(match, tok_hi, 0.0).astype(jnp.bfloat16), dims, preferred_element_type=jnp.float32)
        low = low + lax.dot_general(hit_b, jnp.where(match, tok_lo, 0.0).astype(jnp.bfloat16), dims, preferred_element_type=jnp.float32)
        e = idx_ref[blk:blk + 1, :]
        dx = ((e & 3) - x) & 3
        dy = (((e >> 2) & 3) - y) & 3
        dz = ((e >> 4) - z) & 3
        side = jnp.where(slot >= half, 1, 0)
        rest = slot - side * half
        unit = rest >> 3
        turn = unit + 2 * side
        turn = turn - jnp.where(turn >= 3, 3, 0) - jnp.where(turn >= 6, 3, 0)
        block = jnp.where(turn == 0, dx * 16 + dy * 4 + dz, jnp.where(turn == 1, dy * 16 + dz * 4 + dx, dz * 16 + dx * 4 + dy))
        place = side * (units * CHIPS * SUB) + unit * (CHIPS * SUB) + block * SUB + (rest & 7)
        place_ref[blk:blk + 1, :] = jnp.where(slot < cap, place, CHIPS * cap) * PITCH
    table_ref[...] = (high * CHIPS + low).astype(jnp.int32) * PITCH


def unit_axes(unit, tp):
    x, y, z = my_coords()
    pairs = ((x, 1), (y, SIDE), (z, SIDE * SIDE))
    out = []
    for k in range(3):
        (c0, s0), (c1, s1) = pairs[(unit + k) % 3], pairs[(unit + 2 + k) % 3]
        out.append((c0 * (1 - tp) + c1 * tp, s0 * (1 - tp) + s1 * tp))
    return out


def spread(x_ref, x3, src0, dst0, groups):
    cols = x_ref.shape[-1] // LANES

    def step(g, carry):
        v = x_ref[pl.ds(pl.multiple_of(src0 + g * 16, 16), 16), :].astype(jnp.float32)
        at = (dst0 + g * 16) * PITCH
        for h in range(2):
            for j in range(cols):
                x3[pl.ds(at + h * SUB * PITCH + j, SUB, stride=PITCH), :] = v[h * SUB:(h + 1) * SUB, j * LANES:(j + 1) * LANES]
        return carry

    lax.fori_loop(0, groups, step, 0, unroll=4)


def expert_kernel(cap, units, table, act, w_in, w_out, out, stage, x3, tmp, sent, b1, b2, b3, r1, r2, own, wi, wo, xb, acc, a_sem, s_sem, r_sem, w_s, w_r, w_l, f_s, f_r, f_l):
    tp = lax.axis_index("tp")
    me = lax.axis_index("ep")
    hidden = xb.shape[1]
    cols = hidden // LANES
    slots, chunk = stage.shape[:2]
    pieces = act.shape[0] // chunk
    tall = SIDE * SIDE * SUB
    loads = [pltpu.make_async_copy(act.at[pl.ds(k * chunk, chunk)], stage.at[k % slots], a_sem.at[k]) for k in range(pieces)]
    for copy in loads[:slots]:
        copy.start()

    def dev(ep, core):
        return (0, core, ep)

    def peer(axis, shift):
        pos, stride = axis
        return dev(me + ((pos + shift) % SIDE - pos) * stride, tp)

    axes = [unit_axes(u, tp) for u in range(units)]
    barrier = pltpu.get_barrier_semaphore()
    for axis in axes[0]:
        for shift in (1, 2, 3):
            pl.semaphore_signal(barrier, inc=1, device_id=peer(axis, shift), device_id_type=MESH)
    pl.semaphore_signal(barrier, inc=1, device_id=dev(me, 1 - tp), device_id_type=MESH)
    for k in range(pieces):
        loads[k].wait()
        spread(stage.at[k % slots], x3, 0, k * chunk, chunk // 16)
        if k + slots < pieces:
            loads[k + slots].start()
    pl.semaphore_wait(barrier, 10)

    started = []

    def push(src, dst, send, recv, to):
        copy = pltpu.make_async_remote_copy(src_ref=src, dst_ref=dst, send_sem=send, recv_sem=recv, device_id=to, device_id_type=MESH)
        copy.start()
        started.append(copy)
        return copy

    flights = {}

    def leg(phase, u, axis, sign, src_of, dst_of):
        flights[phase, u] = [
            push(src_of(d), dst_of(d), s_sem.at[phase, u, d - 1], r_sem.at[phase, u, d - 1], peer(axis, sign * d)) for d in (1, 2, 3)
        ]

    def landed(phase, u):
        for copy in flights[phase, u]:
            copy.wait_recv()

    def pick(u, shift, target):
        (a, sa), (b, sb), (c, sc) = axes[u]

        def step(db, carry):
            rows = []
            for dc in range(SIDE):
                e = ((a + shift) % SIDE) * sa + ((b + db) % SIDE) * sb + ((c + dc) % SIDE) * sc
                at = tp * (cap // 2) + u * SUB
                rows += [x3[pl.ds(table[e, at + k], SUB), :] for k in range(SUB)]
            for k, row in enumerate(rows):
                tmp[k * SUB:(k + 1) * SUB, :] = row
            for dc in range(SIDE):
                for j in range(cols):
                    target[db, dc, :, j * LANES:(j + 1) * LANES] = tmp[pl.ds(dc * SUB * SUB + j, SUB, stride=SUB), :].astype(jnp.bfloat16)
            return carry

        lax.fori_loop(0, SIDE, step, 0, unroll=2)

    def d1(u):
        for shift in range(1, SIDE):
            pick(u, shift, sent.at[u, shift - 1])
        leg(0, u, axes[u][0], 1, lambda d: sent.at[u, d - 1], lambda d: b1.at[u, d])
        pick(u, 0, b1.at[u, 0])

    def d2(u):
        landed(0, u)
        leg(1, u, axes[u][1], 1, lambda d: b1.at[u, :, d], lambda d: b2.at[u, d])
        b2[u, 0] = b1[u, :, 0]

    def d3(u):
        landed(1, u)
        leg(2, u, axes[u][2], 1, lambda d: b2.at[u, :, :, d], lambda d: b3.at[u, d])
        b3[u, 0] = b2[u, :, :, 0]

    def half(u, n, d):
        rows = slice(d * tall, (d + 1) * tall)
        pre = jnp.dot(xb[rows, :], wi[n], preferred_element_type=jnp.float32)
        mid = jax.nn.gelu(pre, approximate=True).astype(jnp.bfloat16)
        return jnp.dot(mid, wo[n], preferred_element_type=jnp.float32)

    def first(u):
        landed(2, u)
        for d in range(SIDE):
            rows = slice(d * tall, (d + 1) * tall)
            xb[rows, :] = b3[u, d].astype(jnp.float32).reshape(tall, hidden).astype(jnp.bfloat16)
        for d in range(SIDE):
            acc[d * tall:(d + 1) * tall, :] = half(u, 0, d)

    def second(u):
        for d in range(SIDE):
            total = acc[d * tall:(d + 1) * tall, :] + half(u, 1, d)
            b3[u, d] = total.reshape(SIDE, SIDE, SUB, hidden).astype(jnp.bfloat16)

    def q1(u):
        leg(3, u, axes[u][2], -1, lambda d: b3.at[u, d], lambda d: r1.at[u, d])
        r1[u, 0] = b3[u, 0]

    def q2(u):
        landed(3, u)
        leg(4, u, axes[u][1], -1, lambda d: r1.at[u, :, d], lambda d: r2.at[u, d])
        r2[u, 0] = r1[u, :, 0]

    def q3(u):
        landed(4, u)
        leg(5, u, axes[u][0], -1, lambda d: r2.at[u, :, :, d], lambda d: own.at[u, d])
        own[u, 0] = r2[u, :, :, 0]

    finals = []

    def fin(u):
        landed(5, u)
        keep = pltpu.make_async_copy(own.at[u], out.at[tp, u], f_l.at[u])
        keep.start()
        finals.append(keep)
        flights["fin", u] = [push(own.at[u], out.at[tp, u], f_s.at[u], f_r.at[u], dev(me, 1 - tp))]

    weights = []
    for k, (src, dst) in enumerate(((w_in.at[0], wi.at[tp]), (w_out.at[0], wo.at[tp]))):
        copy = pltpu.make_async_copy(src, dst, w_l.at[k])
        copy.start()
        weights.append(copy)
        flights["w", k] = [push(src, dst, w_s.at[k], w_r.at[k], dev(me, 1 - tp))]

    def ready():
        for copy in weights:
            copy.wait()
        for k in range(2):
            for copy in flights["w", k]:
                copy.wait_recv()

    ops = {"a": d1, "b": d2, "c": d3, "g": first, "h": second, "x": q1, "y": q2, "z": q3, "e": fin}
    for word in ORDER:
        if word == "w":
            ready()
        else:
            ops[word[0]](int(word[1]))
    for u in range(units):
        for copy in flights["fin", u]:
            copy.wait_recv()
    for copy in finals:
        copy.wait()
    for copy in started:
        copy.wait_send()


def combine_kernel(place, gates_hbm, rows, out, stage, x3, tmp, gates, scale, rows_out, gate_sem, in_sem, out_sem):
    total, hidden = rows.shape
    tokens = out.shape[0]
    cols = hidden // LANES
    chunk = 512
    n = total // chunk
    loads = [pltpu.make_async_copy(rows.at[pl.ds(k * chunk, chunk)], stage.at[pl.ds(k * chunk, chunk)], in_sem.at[k]) for k in range(n)]
    gate_load = pltpu.make_async_copy(gates_hbm, gates, gate_sem)
    gate_load.start()
    for c in loads:
        c.start()
    x3[pl.ds(total * PITCH, SUB), :] = jnp.zeros((SUB, LANES), jnp.float32)
    gate_load.wait()
    for k in range(tokens // LANES):
        scale[k * LANES:(k + 1) * LANES, :] = jnp.transpose(jnp.broadcast_to(gates[k:k + 1, :], (LANES, LANES)))
    for k in range(n):
        loads[k].wait()
        spread(stage, x3, k * chunk, k * chunk, chunk // 16)
    stores = []
    for c in range(tokens // chunk):

        def step(g, carry):
            t0 = c * chunk + g * 32
            picked = [x3[pl.ds(place[t0 + k], SUB), :] for k in range(32)]
            for k, row in enumerate(picked):
                tmp[k * SUB:(k + 1) * SUB, :] = row
            for h in range(2):
                gate_a = scale[pl.ds(pl.multiple_of(t0 + h * 16, SUB), SUB), :]
                gate_b = scale[pl.ds(pl.multiple_of(t0 + h * 16 + SUB, SUB), SUB), :]
                for j in range(cols):
                    top = tmp[pl.ds(2 * h * SUB * SUB + j, SUB, stride=SUB), :] * gate_a
                    low = tmp[pl.ds((2 * h + 1) * SUB * SUB + j, SUB, stride=SUB), :] * gate_b
                    rows_out[pl.ds(pl.multiple_of(t0 + h * 16, 16), 16), j * LANES:(j + 1) * LANES] = jnp.concatenate([top, low], axis=0).astype(jnp.bfloat16)
            return carry

        lax.fori_loop(0, chunk // 32, step, 0, unroll=2)
        st = pltpu.make_async_copy(rows_out.at[pl.ds(c * chunk, chunk)], out.at[pl.ds(c * chunk, chunk)], out_sem.at[c])
        st.start()
        stores.append(st)
    for st in stores:
        st.wait()


def solution(mesh):
    tp_size = mesh.shape["tp"]
    vmem = pl.BlockSpec(memory_space=pltpu.VMEM)
    smem = pl.BlockSpec(memory_space=pltpu.SMEM)
    hbm = pl.BlockSpec(memory_space=pl.ANY)
    dma = pltpu.SemaphoreType.DMA

    def local_moe(act_loc, idx_loc, gate_loc, w_in, w_out):
        tokens, hidden = act_loc.shape
        cap = capacity_of(1, tokens, CHIPS, tp_size)
        units = cap // tp_size // SUB
        bf16, f32 = jnp.bfloat16, jnp.float32
        place, table = pl.pallas_call(
            functools.partial(route_kernel, cap, units),
            out_shape=(jax.ShapeDtypeStruct((tokens // LANES, LANES), jnp.int32), jax.ShapeDtypeStruct((CHIPS, cap), jnp.int32)),
            in_specs=[vmem],
            out_specs=(vmem, vmem),
            scratch_shapes=[pltpu.VMEM((tokens // LANES * CHIPS, LANES), bf16)],
            name="route",
        )(idx_loc.reshape(tokens // LANES, LANES))
        cube = (units, SIDE, SIDE, SIDE, SUB, hidden)
        width = w_in.shape[2]
        block_rows = CHIPS * SUB
        chunk = 512
        returned = pl.pallas_call(
            functools.partial(expert_kernel, cap, units),
            out_shape=jax.ShapeDtypeStruct((tp_size,) + cube, bf16),
            in_specs=[smem, hbm, hbm, hbm],
            out_specs=hbm,
            scratch_shapes=[
                pltpu.VMEM((4, chunk, hidden), bf16),
                pltpu.VMEM((tokens * PITCH + SUB, LANES), f32),
                pltpu.VMEM((SIDE * SUB * SUB, LANES), f32),
                pltpu.VMEM((units, SIDE - 1) + cube[2:], bf16),
            ]
            + [pltpu.VMEM(cube, bf16)] * 6
            + [
                pltpu.VMEM((tp_size, hidden, width), bf16),
                pltpu.VMEM((tp_size, width, hidden), bf16),
                pltpu.VMEM((block_rows, hidden), bf16),
                pltpu.VMEM((block_rows, hidden), f32),
                dma((tokens // chunk,)),
                dma((6, units, 3)),
                dma((6, units, 3)),
                dma((2,)),
                dma((2,)),
                dma((2,)),
                dma((units,)),
                dma((units,)),
                dma((units,)),
            ],
            compiler_params=pltpu.CompilerParams(collective_id=0, has_side_effects=True, vmem_limit_bytes=67043328),
            name="expert",
        )(table, act_loc, w_in, w_out)
        total = tp_size * units * block_rows
        return pl.pallas_call(
            combine_kernel,
            out_shape=jax.ShapeDtypeStruct((tokens, hidden), bf16),
            in_specs=[smem, hbm, hbm],
            out_specs=hbm,
            scratch_shapes=[
                pltpu.VMEM((total, hidden), bf16),
                pltpu.VMEM((total * PITCH + SUB, LANES), f32),
                pltpu.VMEM((4 * SUB * SUB, LANES), f32),
                pltpu.VMEM((tokens // LANES, LANES), f32),
                pltpu.VMEM((tokens, LANES), f32),
                pltpu.VMEM((tokens, hidden), bf16),
                dma,
                dma((total // 512,)),
                dma((tokens // 512,)),
            ],
            compiler_params=pltpu.CompilerParams(vmem_limit_bytes=67043328),
            name="combine",
        )(place.reshape(-1), gate_loc.reshape(tokens // LANES, LANES), returned.reshape(total, hidden))

    tok_spec = P(("dp", "ep"), None)
    return jax.shard_map(local_moe, mesh=mesh, in_specs=(tok_spec, tok_spec, tok_spec, P("ep", None, "tp"), P("ep", "tp", None)), out_specs=tok_spec, check_vma=False)
```
